16 devices in a mesh: dp: 4 (over z, y), tp: 4 (over x, core).
Axes of the slice: x: 2, y: 2, z: 2, core: 2. Of those that a mesh axis runs over, the one named last changes fastest.
Arguments:
- x: bfloat16 [96, 64, 5120], P('dp'), parts along dimension 0
- g1: float32 [2, 5120], replicated
- g2: float32 [2, 5120], replicated
- wqkv: bfloat16 [2, 5120, 40, 384], P(None, None, 'tp')
- wo: bfloat16 [2, 5120, 5120], P(None, 'tp')
- w1: bfloat16 [2, 5120, 20480], P(None, None, 'tp')
- w2: bfloat16 [2, 20480, 5120], P(None, 'tp')
Outputs:
- output: bfloat16 [96, 64, 5120], P('dp'), parts along dimension 0
There are 4 independent parts. The reference program is written for one: setup_inputs(seed, part) draws one part's arguments, and reference() takes and returns one part's arrays. A program takes and returns all parts, laid end to end along the dimension named above; an argument that names none is the same for every part.
All inputs are finite; a program needn't handle non-finite values.
Results may differ from the reference program's by a relative error of at most 0.02.
Values are sent between devices in bfloat16 or wider.
A program may use at most 1.5 GiB of HBM per device.

```python
import jax
import jax.numpy as jnp
from jax import lax

BATCH = 24
SEQ = 64
D = 5120
HEADS = 40
FF = 20480
LAYERS = 2

HD = D // HEADS
EPS = 1e-5


def setup_inputs(seed: int = 0, part: int = 0) -> dict:
    kx = jax.random.fold_in(jax.random.key(seed), part)
    k = jax.random.split(jax.random.key(seed + 1), 6)
    x = jax.random.normal(kx, (BATCH, SEQ, D), jnp.float32).astype(jnp.bfloat16)
    g1 = 1.0 + 0.3 * jax.random.normal(k[0], (LAYERS, D), jnp.float32)
    g2 = 1.0 + 0.3 * jax.random.normal(k[1], (LAYERS, D), jnp.float32)
    wqkv = (1.5 * D ** -0.5 * jax.random.normal(k[2], (LAYERS, D, HEADS, 3 * HD), jnp.float32)).astype(jnp.bfloat16)
    wo = (D ** -0.5 * jax.random.normal(k[3], (LAYERS, D, D), jnp.float32)).astype(jnp.bfloat16)
    w1 = (D ** -0.5 * jax.random.normal(k[4], (LAYERS, D, FF), jnp.float32)).astype(jnp.bfloat16)
    w2 = (FF ** -0.5 * jax.random.normal(k[5], (LAYERS, FF, D), jnp.float32)).astype(jnp.bfloat16)
    return {"x": x, "g1": g1, "g2": g2, "wqkv": wqkv, "wo": wo, "w1": w1, "w2": w2}


def _ln(x, g):
    xf = x.astype(jnp.float32)
    mu = jnp.mean(xf, axis=-1, keepdims=True)
    var = jnp.mean(jnp.square(xf - mu), axis=-1, keepdims=True)
    return ((xf - mu) * lax.rsqrt(var + EPS) * g).astype(jnp.bfloat16)


def _attend(item):
    q = item[:, 0]
    k = item[:, 1]
    v = item[:, 2]
    s = jnp.dot(q, k.T, preferred_element_type=jnp.float32) * (HD ** -0.5)
    row = lax.broadcasted_iota(jnp.int32, (SEQ, SEQ), 0)
    col = lax.broadcasted_iota(jnp.int32, (SEQ, SEQ), 1)
    s = jnp.where(row >= col, s, -jnp.inf)
    p = jax.nn.softmax(s, axis=-1).astype(jnp.bfloat16)
    return jnp.dot(p, v, preferred_element_type=jnp.float32).astype(jnp.bfloat16)


def _layer(x, w):
    g1, g2, wqkv, wo, w1, w2 = w
    t = BATCH * SEQ
    h = x.reshape(t, D)
    a = _ln(h, g1)
    qkv = jnp.dot(a, wqkv.reshape(D, 3 * D), preferred_element_type=jnp.float32).astype(jnp.bfloat16)
    qkv = qkv.reshape(BATCH, SEQ, HEADS, 3, HD).transpose(0, 2, 1, 3, 4).reshape(BATCH * HEADS, SEQ, 3, HD)
    o = lax.map(_attend, qkv)
    o = o.reshape(BATCH, HEADS, SEQ, HD).transpose(0, 2, 1, 3).reshape(t, D)
    h = (h.astype(jnp.float32) + jnp.dot(o, wo, preferred_element_type=jnp.float32)).astype(jnp.bfloat16)
    m = jax.nn.gelu(jnp.dot(_ln(h, g2), w1, preferred_element_type=jnp.float32), approximate=True).astype(jnp.bfloat16)
    h = (h.astype(jnp.float32) + jnp.dot(m, w2, preferred_element_type=jnp.float32)).astype(jnp.bfloat16)
    return h.reshape(BATCH, SEQ, D), None


def reference(x, g1, g2, wqkv, wo, w1, w2):
    y, _ = lax.scan(_layer, x, (g1, g2, wqkv, wo, w1, w2))
    return y
```

```python
import functools
import jax
import jax.numpy as jnp
from jax import lax
from jax.experimental import pallas as pl
from jax.experimental.pallas import tpu as pltpu
from jax.sharding import PartitionSpec as P

EPS = 1e-5
F32 = jnp.float32
BF16 = jnp.bfloat16
VLIM = 63 * 1024 * 1024


def _attend_block(q, k, v, mask):
    s = lax.dot_general(q, k, (((1,), (1,)), ((), ())), preferred_element_type=F32) * (128 ** -0.5)
    s = jnp.where(mask, s, -jnp.inf)
    e = jnp.exp(s - jnp.max(s, axis=-1, keepdims=True))
    p = (e / jnp.sum(e, axis=-1, keepdims=True)).astype(BF16)
    return jnp.dot(p, v, preferred_element_type=F32).astype(BF16)


def _attn_kernel(l, t, bs, nq, a0, a1, wq, wo, out_own, out_oth, a, wbuf, qkv, o, sem_a, sem_w):
    j = pl.program_id(0)
    half = t // 2
    seq = 64

    def wcopy(step, slot):
        return [
            pltpu.make_async_copy(wq.at[l, 2 * step + i], wbuf.at[slot, :, pl.ds(384 * i, 384)], sem_w.at[slot, i])
            for i in range(2)
        ]

    @pl.when(j == 0)
    def _():
        c0 = pltpu.make_async_copy(a0, a.at[pl.ds(0, half)], sem_a.at[0])
        c1 = pltpu.make_async_copy(a1, a.at[pl.ds(half, half)], sem_a.at[1])
        c0.start()
        c1.start()
        for cp in wcopy(0, 0):
            cp.start()
        c0.wait()
        c1.wait()

    @pl.when(j < nq)
    def _():
        slot = lax.rem(j, 2)

        @pl.when(j + 1 < nq)
        def _():
            for cp in wcopy(j + 1, 1 - slot):
                cp.start()

        for cp in wcopy(j, slot):
            cp.wait()
        qkv[...] = jnp.dot(a[...], wbuf[slot], preferred_element_type=F32).astype(BF16)
        row = lax.broadcasted_iota(jnp.int32, (bs, bs), 0)
        col = lax.broadcasted_iota(jnp.int32, (bs, bs), 1)
        mask = (row >= col) & (row // seq == col // seq)
        for b in range(t // bs):
            rows = pl.ds(b * bs, bs)
            for i in range(2):
                base = 384 * i
                r = _attend_block(
                    qkv[rows, pl.ds(base, 128)], qkv[rows, pl.ds(base + 128, 128)], qkv[rows, pl.ds(base + 256, 128)], mask
                )
                o[rows, pl.ds(pl.multiple_of(j * 256 + i * 128, 128), 128)] = r

    @pl.when(j >= nq)
    def _():
        r = jnp.dot(o[...], wo[0], preferred_element_type=F32).astype(BF16)
        out_own[...] = r[:half]
        out_oth[...] = r[half:]


def attn_call(l, a0, a1, wq, wo, bn=1024, bs=256):
    half, d = a0.shape
    t = 2 * half
    hl = wq.shape[1]
    nq = hl // 2
    kd = wo.shape[1]
    no = d // bn
    flops = 2 * t * d * hl * 384 + 2 * t * kd * d
    return pl.pallas_call(
        functools.partial(_attn_kernel, l, t, bs, nq),
        grid=(nq + no,),
        in_specs=[
            pl.BlockSpec(memory_space=pl.ANY),
            pl.BlockSpec(memory_space=pl.ANY),
            pl.BlockSpec(memory_space=pl.ANY),
            pl.BlockSpec((1, kd, bn), lambda j: (l, 0, jnp.maximum(j - nq, 0))),
        ],
        out_specs=[pl.BlockSpec((half, bn), lambda j: (0, jnp.maximum(j - nq, 0)))] * 2,
        out_shape=[jax.ShapeDtypeStruct((half, d), BF16)] * 2,
        scratch_shapes=[
            pltpu.VMEM((t, d), BF16),
            pltpu.VMEM((2, d, 768), BF16),
            pltpu.VMEM((t, 768), BF16),
            pltpu.VMEM((t, hl * 128), BF16),
            pltpu.SemaphoreType.DMA((2,)),
            pltpu.SemaphoreType.DMA((2, 2)),
        ],
        compiler_params=pltpu.CompilerParams(dimension_semantics=("arbitrary",), vmem_limit_bytes=VLIM),
        cost_estimate=pl.CostEstimate(flops=flops, bytes_accessed=d * hl * 768 + kd * d * 2 + 4 * t * d, transcendentals=0),
        name=f"attn{l}",
    )(a0, a1, wq, wo)


def _mlp_kernel(l, t, n1, bn, a0, a1, w1, w2, out_own, out_oth, a, m, sem_a):
    j = pl.program_id(0)
    half = t // 2

    @pl.when(j == 0)
    def _():
        c0 = pltpu.make_async_copy(a0, a.at[pl.ds(0, half)], sem_a.at[0])
        c1 = pltpu.make_async_copy(a1, a.at[pl.ds(half, half)], sem_a.at[1])
        c0.start()
        c1.start()
        c0.wait()
        c1.wait()

    @pl.when(j < n1)
    def _():
        r = jnp.dot(a[...], w1[0], preferred_element_type=F32)
        m[:, pl.ds(pl.multiple_of(j * bn, 128), bn)] = jax.nn.gelu(r, approximate=True).astype(BF16)

    @pl.when(j >= n1)
    def _():
        r = jnp.dot(m[...], w2[0], preferred_element_type=F32).astype(BF16)
        out_own[...] = r[:half]
        out_oth[...] = r[half:]


def mlp_call(l, a0, a1, w1, w2, bn=512):
    half, d = a0.shape
    t = 2 * half
    f = w1.shape[2]
    n1, n2 = f // bn, d // bn
    return pl.pallas_call(
        functools.partial(_mlp_kernel, l, t, n1, bn),
        grid=(n1 + n2,),
        in_specs=[
            pl.BlockSpec(memory_space=pl.ANY),
            pl.BlockSpec(memory_space=pl.ANY),
            pl.BlockSpec((1, d, bn), lambda j: (l, 0, jnp.minimum(j, n1 - 1))),
            pl.BlockSpec((1, f, bn), lambda j: (l, 0, jnp.maximum(j - n1, 0))),
        ],
        out_specs=[pl.BlockSpec((half, bn), lambda j: (0, jnp.maximum(j - n1, 0)))] * 2,
        out_shape=[jax.ShapeDtypeStruct((half, d), BF16)] * 2,
        scratch_shapes=[pltpu.VMEM((t, d), BF16), pltpu.VMEM((t, f), BF16), pltpu.SemaphoreType.DMA((2,))],
        compiler_params=pltpu.CompilerParams(dimension_semantics=("arbitrary",), vmem_limit_bytes=VLIM),
        cost_estimate=pl.CostEstimate(flops=4 * t * d * f, bytes_accessed=4 * d * f + 4 * t * d, transcendentals=0),
        name=f"mlp{l}",
    )(a0, a1, w1, w2)


def _norm(x, g):
    mu = jnp.mean(x, axis=-1, keepdims=True)
    xc = x - mu
    var = jnp.mean(jnp.square(xc), axis=-1, keepdims=True)
    return (xc * lax.rsqrt(var + EPS) * g).astype(BF16)


def _post_kernel(off, h, s0, s1, g, h_out, a_out):
    x = (h[...].astype(F32) + (s0[...].astype(F32) + s1[...].astype(F32))).astype(BF16)
    h_out[...] = x
    a_out[...] = _norm(x.astype(F32), g[...])


def post_call(h, base, s0, s1, g, br=64):
    rows, d = s0.shape
    nb = rows // br
    off = jnp.asarray(base // br, jnp.int32).reshape(1)
    return pl.pallas_call(
        _post_kernel,
        grid_spec=pltpu.PrefetchScalarGridSpec(
            num_scalar_prefetch=1,
            grid=(nb,),
            in_specs=[
                pl.BlockSpec((br, d), lambda j, o: (o[0] + j, 0)),
                pl.BlockSpec((br, d), lambda j, o: (j, 0)),
                pl.BlockSpec((br, d), lambda j, o: (j, 0)),
                pl.BlockSpec((1, d), lambda j, o: (0, 0)),
            ],
            out_specs=[pl.BlockSpec((br, d), lambda j, o: (j, 0))] * 2,
        ),
        out_shape=[jax.ShapeDtypeStruct((rows, d), BF16)] * 2,
        compiler_params=pltpu.CompilerParams(dimension_semantics=("arbitrary",), vmem_limit_bytes=VLIM),
        cost_estimate=pl.CostEstimate(flops=10 * rows * d, bytes_accessed=10 * rows * d, transcendentals=0),
        name="post",
    )(off, h, s0, s1, g)


def _ln_kernel(off, h, g, a_out):
    a_out[...] = _norm(h[...].astype(F32), g[...])


def ln_call(h, base, rows, g, br=64):
    d = h.shape[1]
    off = jnp.asarray(base // br, jnp.int32).reshape(1)
    return pl.pallas_call(
        _ln_kernel,
        grid_spec=pltpu.PrefetchScalarGridSpec(
            num_scalar_prefetch=1,
            grid=(rows // br,),
            in_specs=[
                pl.BlockSpec((br, d), lambda j, o: (o[0] + j, 0)),
                pl.BlockSpec((1, d), lambda j, o: (0, 0)),
            ],
            out_specs=pl.BlockSpec((br, d), lambda j, o: (j, 0)),
        ),
        out_shape=jax.ShapeDtypeStruct((rows, d), BF16),
        compiler_params=pltpu.CompilerParams(dimension_semantics=("arbitrary",), vmem_limit_bytes=VLIM),
        cost_estimate=pl.CostEstimate(flops=8 * rows * d, bytes_accessed=4 * rows * d, transcendentals=0),
        name="ln",
    )(off, h, g)


CHUNKS = (8, 8, 8)


def solution(mesh):
    flip_core = [(i, i ^ 1) for i in range(4)]
    flip_chip = [(i, i ^ 2) for i in range(4)]

    def body(x, g1, g2, wqkv, wo, w1, w2):
        b, s, d = x.shape
        layers = wqkv.shape[0]
        c = lax.rem(lax.axis_index("tp"), 2)
        wq = jnp.transpose(wqkv, (0, 2, 1, 3))
        x = x.reshape(b * s, d)
        starts = [sum(CHUNKS[:i]) * s for i in range(len(CHUNKS))]
        halves = [n * s // 2 for n in CHUNKS]
        n = len(CHUNKS)
        res, base, act, oth = [x] * n, [], [], []
        for i in range(n):
            own = starts[i] + c * halves[i]
            base.append(own)
            a = ln_call(x, own, halves[i], g1[0:1])
            act.append(a)
            if i == 0:
                oth.append(ln_call(x, starts[i] + (1 - c) * halves[i], halves[i], g1[0:1]))
            else:
                oth.append(lax.ppermute(a, "tp", flip_core))
        y = jnp.zeros((b * s, d), x.dtype)
        for l in range(layers):
            for kind in range(2):
                for i in range(n):
                    if kind == 0:
                        mine, theirs = attn_call(l, act[i], oth[i], wq, wo)
                    else:
                        mine, theirs = mlp_call(l, act[i], oth[i], w1, w2)
                    got = lax.ppermute(theirs, "tp", flip_core)
                    chip = (mine.astype(F32) + got.astype(F32)).astype(BF16)
                    other = lax.ppermute(chip, "tp", flip_chip)
                    last = l == layers - 1 and kind == 1
                    g = g2[l : l + 1] if kind == 0 else g1[min(l + 1, layers - 1)][None]
                    if last:
                        h = lax.dynamic_slice(res[i], (base[i], 0), (halves[i], d)) if res[i] is x else res[i]
                        h = (h.astype(F32) + (chip.astype(F32) + other.astype(F32))).astype(BF16)
                        ho = lax.ppermute(h, "tp", flip_core)
                        y = lax.dynamic_update_slice(y, h, (starts[i] + c * halves[i], 0))
                        y = lax.dynamic_update_slice(y, ho, (starts[i] + (1 - c) * halves[i], 0))
                    else:
                        res[i], act[i] = post_call(res[i], base[i], chip, other, g)
                        base[i] = 0
                        oth[i] = lax.ppermute(act[i], "tp", flip_core)
        return y.reshape(b, s, d)

    in_specs = (P("dp"), P(), P(), P(None, None, "tp", None), P(None, "tp", None), P(None, None, "tp"), P(None, "tp", None))
    return jax.shard_map(body, mesh=mesh, in_specs=in_specs, out_specs=P("dp"), check_vma=False)
```
